32 devices in a mesh: obs: 2 (over y), bt: 4 (over z), freq: 2 (over x), pol: 2 (over core).
Axes of the slice: x: 2, y: 2, z: 4, core: 2. Of those that a mesh axis runs over, the one named last changes fastest.
Arguments:
- gains: float32 [16, 4, 8, 1984], P(('obs', 'bt', 'pol'), 'freq'), parts along dimension 0, may hold values from -3 to 3
- visibilities: bfloat16 [16, 4, 8, 4096], P('obs', 'freq', None, ('bt', 'pol')), parts along dimension 0, may hold values from -6 to 6
- first_station: int32 [8192], P(('obs', 'bt', 'pol')), parts along dimension 0, may hold values from 0 to 61
- second_station: int32 [8192], P(('obs', 'bt', 'pol')), parts along dimension 0, may hold values from 0 to 61, as said below
- filled_row_count: int32 [16], P(('obs', 'bt', 'pol')), parts along dimension 0, may hold values from 256 to 512
- facet_dir: int32 [16], P('obs'), parts along dimension 0, may hold values from 0 to 7, each once
Outputs:
- corrected: bfloat16 [16, 4, 8, 4096], P('obs', 'freq', None, ('bt', 'pol')), parts along dimension 0
The draws below stay inside these ranges and needn't reach their ends.
There are 2 independent parts, one for each index of `obs`. The reference program is written for one: setup_inputs(seed, part) draws one part's arguments, and reference() takes and returns one part's arrays. A program takes and returns all parts, laid end to end along the dimension named above; each array names one. Nothing has to cross between parts.
Inputs may be any that keep to these rules, and one draw needn't show every extreme that they name: In every row second_station differs from first_station. `facet_dir`: each direction names exactly one facet.
All inputs are finite; a program needn't handle non-finite values.
Results may differ from the reference program's by a relative error of at most 0.001.
Values sent between devices are 32-bit elements; how exact they have to be, the bound alone decides.
A program may use at most 64 MiB of HBM per device.

```python
import jax
import jax.numpy as jnp
from jax import lax

ARRAY_STATIONS = 62
GAIN_SLOT_COUNT = 4
BLOCK_ROW_COUNT = 512
BLOCKS = 8
DIRS = 8
FACETS = 8
CHANS = 4
TIMES = 32
ROWS = 4096


def station_pair(key):
    folded = jax.random.fold_in(key, 17)
    first_key, second_key = jax.random.split(folded)
    first = jax.random.randint(first_key, (ROWS,), 0, ARRAY_STATIONS, dtype=jnp.int32)
    offset = jax.random.randint(second_key, (ROWS,), 1, ARRAY_STATIONS, dtype=jnp.int32)
    return (first, (first + offset) % ARRAY_STATIONS)


def draw_first_station(key, part):
    return station_pair(key)[0]


def draw_second_station(key, part):
    return station_pair(key)[1]


def with_ends(array, stream_key, low, largest):
    longest = array.shape.index(max(array.shape))
    spots = []
    for shift in (0, 1):
        where = [jax.random.randint(jax.random.fold_in(stream_key, axis), (), 0, length) for axis, length in enumerate(array.shape)]
        where[longest] = (where[longest] + shift) % array.shape[longest]
        spots.append(tuple(where))
    return array.at[spots[0]].set(low).at[spots[1]].set(largest)


def levels(rng, shape, pieces, low, largest):
    def one(dim, shards_of):
        heights = jax.random.uniform(jax.random.fold_in(jax.random.fold_in(rng, 6), dim), (shards_of,), jnp.float32, low / len(pieces), largest / len(pieces))
        return jnp.repeat(jnp.exp(heights), shape[dim] // shards_of).reshape((-1,) + (1,) * (len(shape) - dim - 1))

    level = one(*pieces[0])
    for cut in pieces[1:]:
        level = level * one(*cut)
    return level


def centred(own_key, shape, spread, most, cuts=(), kind=jnp.bfloat16):
    level = levels(own_key, shape, cuts, -0.22, 0.18) if cuts else 1.0
    result = jax.random.normal(own_key, shape, jnp.float32) * spread * level
    return jnp.minimum(jnp.maximum(result, -most), most).astype(kind)


def setup_inputs(seed: int = 0, part: int = 0) -> dict:
    streams_of = jax.random.split(jax.random.key(seed), 7)
    part_keys = jax.random.split(jax.random.fold_in(streams_of[6], part), 7)
    gains = centred(part_keys[0], (DIRS, CHANS, 8, TIMES * ARRAY_STATIONS), 0.5, 3.0, ((0, 8), (1, 2)), jnp.float32)
    visibilities = centred(part_keys[1], (FACETS, CHANS, 8, ROWS), 1.0, 6.0, ((1, 2), (3, 8)))
    first_station = draw_first_station(jax.random.fold_in(jax.random.fold_in(streams_of[6], part), 71), part)
    second_station = draw_second_station(jax.random.fold_in(jax.random.fold_in(streams_of[6], part), 71), part)
    filled_row_count = with_ends(jax.random.randint(part_keys[4], (BLOCKS,), BLOCK_ROW_COUNT // 2, BLOCK_ROW_COUNT + 1), jax.random.fold_in(part_keys[4], 1), BLOCK_ROW_COUNT // 2, BLOCK_ROW_COUNT).astype(jnp.int32)
    facet_dir = jax.random.permutation(part_keys[5], DIRS).astype(jnp.int32)
    return dict(gains=gains, visibilities=visibilities, first_station=first_station, second_station=second_station, filled_row_count=filled_row_count, facet_dir=facet_dir)


def entry(values, row_at, col_at):
    return values[..., 2 * row_at + col_at, :], values[..., 4 + 2 * row_at + col_at, :]


def apply_jones(left_matrix, data, right_matrix):
    real_parts = []
    imag_parts = []
    for out_row in (0, 1):
        for out_col in (0, 1):
            total_re = jnp.zeros_like(left_matrix[..., 0, :])
            total_im = jnp.zeros_like(left_matrix[..., 0, :])
            for middle in (0, 1):
                for column in (0, 1):
                    left_re, left_im = entry(left_matrix, out_row, middle)
                    data_re, data_im = entry(data, middle, column)
                    right_re, right_im = entry(right_matrix, out_col, column)
                    prod_re = left_re * data_re - left_im * data_im
                    prod_im = left_re * data_im + left_im * data_re
                    total_re = total_re + prod_re * right_re + prod_im * right_im
                    total_im = total_im + prod_im * right_re - prod_re * right_im
            real_parts.append(total_re)
            imag_parts.append(total_im)
    return jnp.stack(real_parts + imag_parts, axis=-2)


def slot_blend_weight(antenna, block_rows, slots, stations):
    row_ids = jnp.arange(block_rows, dtype=jnp.int32)
    per_slot = block_rows // slots
    row_slot = row_ids // per_slot
    fraction = ((row_ids % per_slot).astype(jnp.float32) + 0.5) / per_slot
    slot_ids = jnp.arange(slots + 1, dtype=jnp.int32)[:, None, None]
    station_ids = jnp.arange(stations, dtype=jnp.int32)[None, :, None]
    time_weight = jnp.where(slot_ids == row_slot[None, None, :], 1.0 - fraction, 0.0 * fraction)
    time_weight = time_weight + jnp.where(slot_ids == row_slot[None, None, :] + 1, fraction, 0.0 * fraction)
    station_mask = (station_ids == antenna[None, None, :]).astype(jnp.float32)
    weights_table = time_weight * station_mask
    return weights_table.reshape((slots + 1) * stations, block_rows)


def apply_correction(gain_window, block_visibilities, first_station_gain, second_station_gain, filled_rows):
    block_rows = block_visibilities.shape[3]
    left_matrix = jnp.einsum("hsxv,va->hsxa", gain_window, slot_blend_weight(first_station_gain, block_rows, GAIN_SLOT_COUNT, ARRAY_STATIONS), precision=lax.Precision.HIGHEST)
    right_matrix = jnp.einsum("hsxv,va->hsxa", gain_window, slot_blend_weight(second_station_gain, block_rows, GAIN_SLOT_COUNT, ARRAY_STATIONS), precision=lax.Precision.HIGHEST)
    product = apply_jones(left_matrix, block_visibilities.astype(jnp.float32), right_matrix)
    live_mask = jnp.arange(block_rows, dtype=jnp.int32) < filled_rows
    return jnp.where(live_mask, product, 0.0 * product).astype(jnp.bfloat16)


def reference(gains, visibilities, first_station, second_station, filled_row_count, facet_dir):
    onehot = (facet_dir[:, None] == jnp.arange(DIRS, dtype=jnp.int32)[None, :]).astype(jnp.float32)
    chosen = jnp.einsum("fd,dckn->fckn", onehot, gains, precision=lax.Precision.HIGHEST)
    final_slot = chosen[..., (TIMES - 1) * ARRAY_STATIONS:]
    extended = jnp.concatenate([chosen, final_slot], axis=3)

    def one_block(block_index):
        gain_window = lax.dynamic_slice_in_dim(extended, block_index * (GAIN_SLOT_COUNT * ARRAY_STATIONS), (GAIN_SLOT_COUNT + 1) * ARRAY_STATIONS, 3)
        block_visibilities = lax.dynamic_slice_in_dim(visibilities, block_index * BLOCK_ROW_COUNT, BLOCK_ROW_COUNT, 3)
        first_station_gain = lax.dynamic_slice_in_dim(first_station, block_index * BLOCK_ROW_COUNT, BLOCK_ROW_COUNT, 0)
        second_station_gain = lax.dynamic_slice_in_dim(second_station, block_index * BLOCK_ROW_COUNT, BLOCK_ROW_COUNT, 0)
        return apply_correction(gain_window, block_visibilities, first_station_gain, second_station_gain, filled_row_count[block_index])

    blocks_out = lax.map(one_block, jnp.arange(BLOCKS, dtype=jnp.int32))
    blocks_out = jnp.moveaxis(blocks_out, 0, 3)
    return blocks_out.reshape(FACETS, CHANS, 8, ROWS)
```

```python
import functools

import jax
import jax.numpy as jnp
from jax import lax
from jax.experimental import pallas as pl
from jax.experimental.pallas import tpu as pltpu
from jax.sharding import PartitionSpec as P

ARRAY_STATIONS = 62
GAIN_SLOT_COUNT = 4
MESH = pl.DeviceIdType.MESH
LANES = 128
HALF = 64
COMPS = 8
F32 = jnp.float32
BF16 = jnp.bfloat16


def pair_tile(left, right):
    gap = jnp.zeros((left.shape[0], HALF - ARRAY_STATIONS), F32)
    return jnp.concatenate([left, gap, right, gap], axis=1)


def complex_dot(pairs, conj):
    re = im = None
    for (ar, ai), (br, bi) in pairs:
        if conj:
            pr = ar * br + ai * bi
            pi = ai * br - ar * bi
        else:
            pr = ar * br - ai * bi
            pi = ar * bi + ai * br
        re = pr if re is None else re + pr
        im = pi if im is None else im + pi
    return re, im


def jones(left, data, right):
    a = lambda m, i, j: (m[2 * i + j], m[4 + 2 * i + j])
    mid = {}
    for i in (0, 1):
        for j in (0, 1):
            mid[i, j] = complex_dot(
                [(a(left, i, t), a(data, t, j)) for t in (0, 1)], False
            )
    out = [None] * COMPS
    for i in (0, 1):
        for j in (0, 1):
            re, im = complex_dot(
                [(mid[i, t], a(right, j, t)) for t in (0, 1)], True
            )
            out[2 * i + j], out[4 + 2 * i + j] = re, im
    return out


def kernel(
    n,
    pols,
    gains_hbm,
    vis_hbm,
    first_hbm,
    second_hbm,
    filled_hbm,
    dir_hbm,
    out_ref,
    gains,
    vis,
    stations,
    filled,
    dirs,
    send,
    recv,
    table,
    planar,
    in_sem,
    send_sem,
    recv_sem,
):
    facets, chans, comps, rows = vis.shape
    slots = GAIN_SLOT_COUNT
    per_slot = rows // slots
    tiles = send.shape[1] // COMPS
    ck = chans * comps
    me = lax.axis_index("bt") * pols + lax.axis_index("pol")

    def where_is(block):
        return {"bt": block // pols, "pol": lax.rem(block, pols)}

    copies = [
        pltpu.make_async_copy(src, dst, in_sem.at[i])
        for i, (src, dst) in enumerate(
            [
                (gains_hbm, gains),
                (dir_hbm, dirs),
                (filled_hbm, filled),
                (first_hbm, stations.at[0]),
                (second_hbm, stations.at[1]),
                (vis_hbm, vis),
            ]
        )
    ]
    for copy in copies:
        copy.start()

    barrier = pltpu.get_barrier_semaphore()
    for off in range(1, n):
        pl.semaphore_signal(
            barrier,
            inc=1,
            device_id=where_is(lax.rem(me + off, n)),
            device_id_type=MESH,
        )

    copies[0].wait()
    lane = lax.broadcasted_iota(jnp.int32, (COMPS, LANES), 1)
    st = ARRAY_STATIONS

    def slot_of(c, t):
        t = min(t, n * slots - 1)
        return gains[0, c, :, t * st : (t + 1) * st]

    for b in range(n):
        at = 0
        for pair in range(slots // 2):
            for c in range(chans):
                t = b * slots + 2 * pair
                send[b, at * COMPS : (at + 1) * COMPS, :] = pair_tile(
                    slot_of(c, t), slot_of(c, t + 1)
                )
                at += 1
        for c in range(0, chans, 2):
            t = (b + 1) * slots
            send[b, at * COMPS : (at + 1) * COMPS, :] = pair_tile(
                slot_of(c, t), slot_of(min(c + 1, chans - 1), t)
            )
            at += 1

    pl.semaphore_wait(barrier, n - 1)
    slab = tiles * COMPS

    def remote(block, slot_dev):
        return pltpu.make_async_remote_copy(
            src_ref=send.at[block],
            dst_ref=recv.at[pl.ds(pl.multiple_of(slot_dev * slab, 8), slab), :],
            send_sem=send_sem.at[block],
            recv_sem=recv_sem.at[slot_dev],
            device_id=where_is(block),
            device_id_type=MESH,
        )

    order = sorted(range(1, n), key=lambda off: abs(off - n // 2))
    for off in order:
        remote(lax.rem(me + off, n), me).start()
    recv[pl.ds(pl.multiple_of(me * slab, 8), slab), :] = send[me]

    for copy in copies[1:5]:
        copy.wait()
    row = lax.broadcasted_iota(jnp.int32, (LANES, per_slot), 0)
    col = lax.broadcasted_iota(jnp.int32, (LANES, per_slot), 1)
    station = lax.rem(row, HALF)
    lower = row < HALF
    frac = (col.astype(F32) + 0.5) / per_slot
    live_rows = filled[0]
    for s in range(slots):
        now, then = 1.0 - frac, frac
        weight = jnp.where(lower, now, then) if s % 2 == 0 else jnp.where(lower, then, now)
        live = (col + s * per_slot) < live_rows
        first = stations[0, s : s + 1, :]
        second = stations[1, s : s + 1, :]
        lt = jnp.where((station == first) & live, weight, 0.0)
        rt = jnp.where(station == second, weight, 0.0)
        both = jnp.concatenate([lt, rt], axis=1).astype(BF16)
        table[s, 0:LANES, :] = both
        table[s, LANES : 2 * LANES, :] = both

    copies[5].wait()
    total = facets * ck
    prow = lax.broadcasted_iota(jnp.int32, (total, total), 0)
    pcol = lax.broadcasted_iota(jnp.int32, (total, total), 1)
    facet_of = pcol // ck
    dir_of = jnp.zeros_like(pcol)
    for f in range(facets):
        dir_of = jnp.where(facet_of == f, dirs[f], dir_of)
    target = lax.rem(pcol, ck) * facets + dir_of
    perm32 = jnp.where(prow == target, 1.0, 0.0)
    perm = perm32.astype(BF16)
    unperm = perm32.T.astype(BF16)
    flat = vis[...].astype(F32).reshape(total, rows).astype(BF16)
    planar[...] = jnp.dot(perm, flat, preferred_element_type=F32)

    for off in order:
        remote(me, lax.rem(me - off + n, n)).wait_recv()

    def gathered(at, c_rot):
        planes = []
        for k in range(comps):
            plane = recv[pl.ds(at * COMPS + k, facets, stride=slab), :]
            if c_rot:
                plane = pltpu.roll(plane, HALF, 1)
            planes.append(plane)
        return planes

    def stacked(pair):
        planes = []
        for c in range(chans):
            if pair < slots // 2:
                planes += gathered(pair * chans + c, False)
            else:
                planes += gathered((slots // 2) * chans + c // 2, c % 2 == 1)
        return jnp.concatenate(planes, axis=0)

    pairs = [stacked(p) for p in range(slots // 2 + 1)]
    in_low = lax.broadcasted_iota(jnp.int32, (total, LANES), 1) < HALF
    done = []
    for s in range(slots):
        made = []
        x = pairs[s // 2]
        if s % 2 == 1:
            x = jnp.where(in_low, pairs[s // 2 + 1], x)
        hi = x.astype(BF16)
        lo = (x - hi.astype(F32)).astype(BF16)
        spread = jnp.dot(
            jnp.concatenate([hi, lo], axis=1), table[s], preferred_element_type=F32
        )
        for c in range(chans):
            take = lambda k: slice((c * comps + k) * facets, (c * comps + k + 1) * facets)
            left = [spread[take(k), 0:per_slot] for k in range(comps)]
            right = [spread[take(k), per_slot:] for k in range(comps)]
            data = [planar[take(k), s * per_slot : (s + 1) * per_slot] for k in range(comps)]
            made += jones(left, data, right)
        done.append(jnp.concatenate(made, axis=0).astype(BF16))
        if s % 2 == 1:
            wide = jnp.concatenate(done, axis=1)
            done = []
            back = jnp.dot(unperm, wide, preferred_element_type=F32)
            for f in range(facets):
                for c in range(chans):
                    at = (f * chans + c) * comps
                    out_ref[f, c, :, (s - 1) * per_slot : (s + 1) * per_slot] = back[
                        at : at + comps, :
                    ].astype(BF16)

    for off in order:
        remote(lax.rem(me + off, n), me).wait_send()


def shards(gains, visibilities, first_station, second_station, filled_row_count, facet_dir):
    n = lax.axis_size(("bt", "pol"))
    pols = lax.axis_size("pol")
    facets, chans, comps, rows = visibilities.shape
    slots = GAIN_SLOT_COUNT
    tiles = (slots // 2) * chans + (chans + 1) // 2
    total = facets * chans * comps
    anywhere = pl.BlockSpec(memory_space=pl.ANY)
    return pl.pallas_call(
        functools.partial(kernel, n, pols),
        out_shape=jax.ShapeDtypeStruct(visibilities.shape, BF16),
        in_specs=[anywhere] * 6,
        out_specs=pl.BlockSpec(memory_space=pltpu.VMEM),
        scratch_shapes=[
            pltpu.VMEM(gains.shape, F32),
            pltpu.VMEM(visibilities.shape, BF16),
            pltpu.VMEM((2, slots, rows // slots), jnp.int32),
            pltpu.SMEM(filled_row_count.shape, jnp.int32),
            pltpu.SMEM(facet_dir.shape, jnp.int32),
            pltpu.VMEM((n, tiles * COMPS, LANES), F32),
            pltpu.VMEM((n * tiles * COMPS, LANES), F32),
            pltpu.VMEM((slots, 2 * LANES, 2 * (rows // slots)), BF16),
            pltpu.VMEM((total, rows), F32),
            pltpu.SemaphoreType.DMA((6,)),
            pltpu.SemaphoreType.DMA((n,)),
            pltpu.SemaphoreType.DMA((n,)),
        ],
        compiler_params=pltpu.CompilerParams(collective_id=0, has_side_effects=True),
        name="jones",
    )(
        gains,
        visibilities,
        first_station.reshape(slots, rows // slots),
        second_station.reshape(slots, rows // slots),
        filled_row_count,
        facet_dir,
    )


def solution(mesh):
    return jax.shard_map(
        shards,
        mesh=mesh,
        in_specs=(
            P(("obs", "bt", "pol"), "freq", None, None),
            P("obs", "freq", None, ("bt", "pol")),
            P(("obs", "bt", "pol")),
            P(("obs", "bt", "pol")),
            P(("obs", "bt", "pol")),
            P("obs"),
        ),
        out_specs=P("obs", "freq", None, ("bt", "pol")),
        check_vma=False,
    )
```

```python
import functools

import jax
import jax.numpy as jnp
from jax import lax
from jax.experimental import pallas as pl
from jax.experimental.pallas import tpu as pltpu
from jax.sharding import PartitionSpec as P

ARRAY_STATIONS = 62
GAIN_SLOT_COUNT = 4
MESH = pl.DeviceIdType.MESH
LANES = 128
HALF = 64
COMPS = 8
F32 = jnp.float32
BF16 = jnp.bfloat16


def pair_tile(left, right):
    gap = jnp.zeros((left.shape[0], HALF - ARRAY_STATIONS), F32)
    return jnp.concatenate([left, gap, right, gap], axis=1)


def complex_dot(pairs, conj):
    re = im = None
    for (ar, ai), (br, bi) in pairs:
        if conj:
            pr = ar * br + ai * bi
            pi = ai * br - ar * bi
        else:
            pr = ar * br - ai * bi
            pi = ar * bi + ai * br
        re = pr if re is None else re + pr
        im = pi if im is None else im + pi
    return re, im


def jones(left, data, right):
    a = lambda m, i, j: (m[2 * i + j], m[4 + 2 * i + j])
    mid = {}
    for i in (0, 1):
        for j in (0, 1):
            mid[i, j] = complex_dot(
                [(a(left, i, t), a(data, t, j)) for t in (0, 1)], False
            )
    out = [None] * COMPS
    for i in (0, 1):
        for j in (0, 1):
            re, im = complex_dot(
                [(mid[i, t], a(right, j, t)) for t in (0, 1)], True
            )
            out[2 * i + j], out[4 + 2 * i + j] = re, im
    return out


def kernel(
    n,
    pols,
    gains_hbm,
    vis_hbm,
    first_hbm,
    second_hbm,
    filled_hbm,
    dir_hbm,
    out_ref,
    gains,
    vis,
    stations,
    filled,
    dirs,
    send,
    recv,
    table,
    planar,
    in_sem,
    send_sem,
    recv_sem,
):
    facets, chans, comps, rows = vis.shape
    slots = GAIN_SLOT_COUNT
    per_slot = rows // slots
    tiles = send.shape[1] // COMPS
    ck = chans * comps
    me = lax.axis_index("bt") * pols + lax.axis_index("pol")

    def where_is(block):
        return {"bt": block // pols, "pol": lax.rem(block, pols)}

    copies = [
        pltpu.make_async_copy(src, dst, in_sem.at[i])
        for i, (src, dst) in enumerate(
            [
                (gains_hbm, gains),
                (dir_hbm, dirs),
                (filled_hbm, filled),
                (first_hbm, stations.at[0]),
                (second_hbm, stations.at[1]),
                (vis_hbm, vis),
            ]
        )
    ]
    for copy in copies:
        copy.start()

    barrier = pltpu.get_barrier_semaphore()
    for off in range(1, n):
        pl.semaphore_signal(
            barrier,
            inc=1,
            device_id=where_is(lax.rem(me + off, n)),
            device_id_type=MESH,
        )

    copies[0].wait()
    lane = lax.broadcasted_iota(jnp.int32, (COMPS, LANES), 1)
    st = ARRAY_STATIONS

    def slot_of(c, t):
        t = min(t, n * slots - 1)
        return gains[0, c, :, t * st : (t + 1) * st]

    for b in range(n):
        at = 0
        for pair in range(slots // 2):
            for c in range(chans):
                t = b * slots + 2 * pair
                send[b, at * COMPS : (at + 1) * COMPS, :] = pair_tile(
                    slot_of(c, t), slot_of(c, t + 1)
                )
                at += 1
        for c in range(0, chans, 2):
            t = (b + 1) * slots
            send[b, at * COMPS : (at + 1) * COMPS, :] = pair_tile(
                slot_of(c, t), slot_of(min(c + 1, chans - 1), t)
            )
            at += 1

    pl.semaphore_wait(barrier, n - 1)
    slab = tiles * COMPS

    def remote(block, slot_dev):
        return pltpu.make_async_remote_copy(
            src_ref=send.at[block],
            dst_ref=recv.at[pl.ds(pl.multiple_of(slot_dev * slab, 8), slab), :],
            send_sem=send_sem.at[block],
            recv_sem=recv_sem.at[slot_dev],
            device_id=where_is(block),
            device_id_type=MESH,
        )

    order = sorted(range(1, n), key=lambda off: abs(off - n // 2))
    for off in order:
        remote(lax.rem(me + off, n), me).start()
    recv[pl.ds(pl.multiple_of(me * slab, 8), slab), :] = send[me]

    for copy in copies[1:5]:
        copy.wait()
    row = lax.broadcasted_iota(jnp.int32, (LANES, per_slot), 0)
    col = lax.broadcasted_iota(jnp.int32, (LANES, per_slot), 1)
    station = lax.rem(row, HALF)
    lower = row < HALF
    frac = (col.astype(F32) + 0.5) / per_slot
    live_rows = filled[0]
    for s in range(slots):
        now, then = 1.0 - frac, frac
        weight = jnp.where(lower, now, then) if s % 2 == 0 else jnp.where(lower, then, now)
        live = (col + s * per_slot) < live_rows
        first = stations[0, s : s + 1, :]
        second = stations[1, s : s + 1, :]
        lt = jnp.where((station == first) & live, weight, 0.0)
        rt = jnp.where(station == second, weight, 0.0)
        both = jnp.concatenate([lt, rt], axis=1).astype(BF16)
        table[s, 0:LANES, :] = both
        table[s, LANES : 2 * LANES, :] = both

    copies[5].wait()
    total = facets * ck
    prow = lax.broadcasted_iota(jnp.int32, (total, total), 0)
    pcol = lax.broadcasted_iota(jnp.int32, (total, total), 1)
    facet_of = pcol // ck
    dir_of = jnp.zeros_like(pcol)
    for f in range(facets):
        dir_of = jnp.where(facet_of == f, dirs[f], dir_of)
    target = lax.rem(pcol, ck) * facets + dir_of
    perm32 = jnp.where(prow == target, 1.0, 0.0)
    perm = perm32.astype(BF16)
    unperm = perm32.T.astype(BF16)
    flat = vis[...].astype(F32).reshape(total, rows).astype(BF16)
    planar[...] = jnp.dot(perm, flat, preferred_element_type=F32)

    for off in order:
        remote(me, lax.rem(me - off + n, n)).wait_recv()

    def gathered(at, c_rot):
        planes = []
        for k in range(comps):
            plane = recv[pl.ds(at * COMPS + k, facets, stride=slab), :]
            if c_rot:
                plane = pltpu.roll(plane, HALF, 1)
            planes.append(plane)
        return planes

    def stacked(pair):
        planes = []
        for c in range(chans):
            if pair < slots // 2:
                planes += gathered(pair * chans + c, False)
            else:
                planes += gathered((slots // 2) * chans + c // 2, c % 2 == 1)
        return jnp.concatenate(planes, axis=0)

    pairs = [stacked(p) for p in range(slots // 2 + 1)]
    in_low = lax.broadcasted_iota(jnp.int32, (total, LANES), 1) < HALF
    done = []
    for s in range(slots):
        made = []
        x = pairs[s // 2]
        if s % 2 == 1:
            x = jnp.where(in_low, pairs[s // 2 + 1], x)
        hi = x.astype(BF16)
        lo = (x - hi.astype(F32)).astype(BF16)
        spread = jnp.dot(
            jnp.concatenate([hi, lo], axis=1), table[s], preferred_element_type=F32
        )
        for c in range(chans):
            take = lambda k: slice((c * comps + k) * facets, (c * comps + k + 1) * facets)
            left = [spread[take(k), 0:per_slot] for k in range(comps)]
            right = [spread[take(k), per_slot:] for k in range(comps)]
            data = [planar[take(k), s * per_slot : (s + 1) * per_slot] for k in range(comps)]
            made += jones(left, data, right)
        done.append(jnp.concatenate(made, axis=0).astype(BF16))
        if s % 2 == 1:
            wide = jnp.concatenate(done, axis=1)
            done = []
            back = jnp.dot(unperm, wide, preferred_element_type=F32)
            for f in range(facets):
                for c in range(chans):
                    at = (f * chans + c) * comps
                    out_ref[f, c, :, (s - 1) * per_slot : (s + 1) * per_slot] = back[
                        at : at + comps, :
                    ].astype(BF16)

    for off in order:
        remote(lax.rem(me + off, n), me).wait_send()


def shards(gains, visibilities, first_station, second_station, filled_row_count, facet_dir):
    n = lax.axis_size(("bt", "pol"))
    pols = lax.axis_size("pol")
    facets, chans, comps, rows = visibilities.shape
    slots = GAIN_SLOT_COUNT
    tiles = (slots // 2) * chans + (chans + 1) // 2
    total = facets * chans * comps
    anywhere = pl.BlockSpec(memory_space=pl.ANY)
    return pl.pallas_call(
        functools.partial(kernel, n, pols),
        out_shape=pltpu.VMEM(visibilities.shape, BF16),
        in_specs=[anywhere] * 6,
        out_specs=pl.BlockSpec(memory_space=pltpu.VMEM),
        scratch_shapes=[
            pltpu.VMEM(gains.shape, F32),
            pltpu.VMEM(visibilities.shape, BF16),
            pltpu.VMEM((2, slots, rows // slots), jnp.int32),
            pltpu.SMEM(filled_row_count.shape, jnp.int32),
            pltpu.SMEM(facet_dir.shape, jnp.int32),
            pltpu.VMEM((n, tiles * COMPS, LANES), F32),
            pltpu.VMEM((n * tiles * COMPS, LANES), F32),
            pltpu.VMEM((slots, 2 * LANES, 2 * (rows // slots)), BF16),
            pltpu.VMEM((total, rows), F32),
            pltpu.SemaphoreType.DMA((6,)),
            pltpu.SemaphoreType.DMA((n,)),
            pltpu.SemaphoreType.DMA((n,)),
        ],
        compiler_params=pltpu.CompilerParams(collective_id=0, has_side_effects=True),
        name="jones",
    )(
        gains,
        visibilities,
        first_station.reshape(slots, rows // slots),
        second_station.reshape(slots, rows // slots),
        filled_row_count,
        facet_dir,
    )


def solution(mesh):
    return jax.shard_map(
        shards,
        mesh=mesh,
        in_specs=(
            P(("obs", "bt", "pol"), "freq", None, None),
            P("obs", "freq", None, ("bt", "pol")),
            P(("obs", "bt", "pol")),
            P(("obs", "bt", "pol")),
            P(("obs", "bt", "pol")),
            P("obs"),
        ),
        out_specs=P("obs", "freq", None, ("bt", "pol")),
        check_vma=False,
    )
```

```python
import functools

import jax
import jax.numpy as jnp
from jax import lax
from jax.experimental import pallas as pl
from jax.experimental.pallas import tpu as pltpu
from jax.sharding import PartitionSpec as P

ARRAY_STATIONS = 62
GAIN_SLOT_COUNT = 4
MESH = pl.DeviceIdType.MESH
LANES = 128
HALF = 64
COMPS = 8
F32 = jnp.float32
BF16 = jnp.bfloat16


def pair_tile(left, right):
    gap = jnp.zeros((left.shape[0], HALF - ARRAY_STATIONS), F32)
    return jnp.concatenate([left, gap, right, gap], axis=1)


def complex_dot(pairs, conj):
    re = im = None
    for (ar, ai), (br, bi) in pairs:
        if conj:
            pr = ar * br + ai * bi
            pi = ai * br - ar * bi
        else:
            pr = ar * br - ai * bi
            pi = ar * bi + ai * br
        re = pr if re is None else re + pr
        im = pi if im is None else im + pi
    return re, im


def jones(left, data, right):
    a = lambda m, i, j: (m[2 * i + j], m[4 + 2 * i + j])
    mid = {}
    for i in (0, 1):
        for j in (0, 1):
            mid[i, j] = complex_dot(
                [(a(left, i, t), a(data, t, j)) for t in (0, 1)], False
            )
    out = [None] * COMPS
    for i in (0, 1):
        for j in (0, 1):
            re, im = complex_dot(
                [(mid[i, t], a(right, j, t)) for t in (0, 1)], True
            )
            out[2 * i + j], out[4 + 2 * i + j] = re, im
    return out


def kernel(
    n,
    pols,
    gains_hbm,
    vis_hbm,
    first_hbm,
    second_hbm,
    filled_hbm,
    dir_hbm,
    out_ref,
    gains,
    vis,
    stations,
    filled,
    dirs,
    send,
    recv,
    table,
    planar,
    in_sem,
    send_sem,
    recv_sem,
):
    facets, chans, comps, rows = vis.shape
    slots = GAIN_SLOT_COUNT
    per_slot = rows // slots
    tiles = send.shape[0] // COMPS // n
    ck = chans * comps
    bts = n // pols
    my_bt, my_pol = lax.axis_index("bt"), lax.axis_index("pol")
    me = my_bt * pols + my_pol
    steps = [(dz, dp) for dz in range(bts) for dp in range(pols) if dz or dp]
    steps.sort(key=lambda step: (step[0] == 0, abs(2 * step[0] - bts)))
    peers = [
        (lax.rem(my_bt + dz, bts), lax.rem(my_pol + dp, pols)) for dz, dp in steps
    ]

    copies = [
        pltpu.make_async_copy(src, dst, in_sem.at[i])
        for src, dst, i in [
            (gains_hbm, gains, 0),
            (first_hbm, stations.at[0], 1),
            (second_hbm, stations.at[1], 1),
            (dir_hbm, dirs, 2),
            (filled_hbm, filled, 3),
            (vis_hbm, vis, 4),
        ]
    ]
    copies[0].start()
    barrier = pltpu.get_barrier_semaphore()
    for bt, pol in peers:
        pl.semaphore_signal(
            barrier, inc=1, device_id={"bt": bt, "pol": pol}, device_id_type=MESH
        )
    for copy in copies[1:]:
        copy.start()

    copies[0].wait()
    lane = lax.broadcasted_iota(jnp.int32, (COMPS, LANES), 1)
    st = ARRAY_STATIONS

    def slot_of(c, t):
        t = min(t, n * slots - 1)
        return gains[0, c, :, t * st : (t + 1) * st]

    for b in range(n):
        at = 0
        for pair in range(slots // 2):
            for c in range(chans):
                t = b * slots + 2 * pair
                send[pl.ds((b * tiles + at) * COMPS, COMPS), :] = pair_tile(
                    slot_of(c, t), slot_of(c, t + 1)
                )
                at += 1
        for c in range(0, chans, 2):
            t = (b + 1) * slots
            send[pl.ds((b * tiles + at) * COMPS, COMPS), :] = pair_tile(
                slot_of(c, t), slot_of(min(c + 1, chans - 1), t)
            )
            at += 1

    pl.semaphore_wait(barrier, n - 1)
    slab = tiles * COMPS

    mine = pl.ds(pl.multiple_of(me * slab, 8), slab)
    for bt, pol in peers:
        pltpu.make_async_remote_copy(
            src_ref=send.at[pl.ds(pl.multiple_of((bt * pols + pol) * slab, 8), slab), :],
            dst_ref=recv.at[mine, :],
            send_sem=send_sem,
            recv_sem=recv_sem,
            device_id={"bt": bt, "pol": pol},
            device_id_type=MESH,
        ).start()
    recv[mine, :] = send[mine, :]

    pltpu.make_async_copy(stations, stations, in_sem.at[1]).wait()
    copies[3].wait()
    copies[4].wait()
    row = lax.broadcasted_iota(jnp.int32, (LANES, per_slot), 0)
    col = lax.broadcasted_iota(jnp.int32, (LANES, per_slot), 1)
    station = lax.rem(row, HALF)
    lower = row < HALF
    frac = (col.astype(F32) + 0.5) / per_slot
    live_rows = filled[0]
    for s in range(slots):
        now, then = 1.0 - frac, frac
        weight = jnp.where(lower, now, then) if s % 2 == 0 else jnp.where(lower, then, now)
        live = (col + s * per_slot) < live_rows
        first = stations[0, s : s + 1, :]
        second = stations[1, s : s + 1, :]
        lt = jnp.where((station == first) & live, weight, 0.0)
        rt = jnp.where(station == second, weight, 0.0)
        both = jnp.concatenate([lt, rt], axis=1).astype(BF16)
        table[s, 0:LANES, :] = both
        table[s, LANES : 2 * LANES, :] = both

    copies[5].wait()
    total = facets * ck
    prow = lax.broadcasted_iota(jnp.int32, (total, total), 0)
    pcol = lax.broadcasted_iota(jnp.int32, (total, total), 1)
    facet_of = pcol // ck
    dir_of = jnp.zeros_like(pcol)
    for f in range(facets):
        dir_of = jnp.where(facet_of == f, dirs[f], dir_of)
    target = lax.rem(pcol, ck) * facets + dir_of
    perm32 = jnp.where(prow == target, 1.0, 0.0)
    perm = perm32.astype(BF16)
    unperm = perm32.T.astype(BF16)
    flat = vis[...].astype(F32).reshape(total, rows).astype(BF16)
    planar[...] = jnp.dot(perm, flat, preferred_element_type=F32)

    arrived = recv.at[pl.ds(0, (n - 1) * slab), :]
    pltpu.make_async_copy(arrived, arrived, recv_sem).wait()

    def gathered(at, c_rot):
        planes = []
        for k in range(comps):
            plane = recv[pl.ds(at * COMPS + k, facets, stride=slab), :]
            if c_rot:
                plane = pltpu.roll(plane, HALF, 1)
            planes.append(plane)
        return planes

    def stacked(pair):
        planes = []
        for c in range(chans):
            if pair < slots // 2:
                planes += gathered(pair * chans + c, False)
            else:
                planes += gathered((slots // 2) * chans + c // 2, c % 2 == 1)
        return jnp.concatenate(planes, axis=0)

    pairs = [stacked(p) for p in range(slots // 2 + 1)]
    in_low = lax.broadcasted_iota(jnp.int32, (total, LANES), 1) < HALF
    done = []
    for s in range(slots):
        made = []
        x = pairs[s // 2]
        if s % 2 == 1:
            x = jnp.where(in_low, pairs[s // 2 + 1], x)
        hi = x.astype(BF16)
        lo = (x - hi.astype(F32)).astype(BF16)
        spread = jnp.dot(
            jnp.concatenate([hi, lo], axis=1), table[s], preferred_element_type=F32
        )
        for c in range(chans):
            take = lambda k: slice((c * comps + k) * facets, (c * comps + k + 1) * facets)
            left = [spread[take(k), 0:per_slot] for k in range(comps)]
            right = [spread[take(k), per_slot:] for k in range(comps)]
            data = [planar[take(k), s * per_slot : (s + 1) * per_slot] for k in range(comps)]
            made += jones(left, data, right)
        done.append(jnp.concatenate(made, axis=0).astype(BF16))
        if s % 2 == 1:
            wide = jnp.concatenate(done, axis=1)
            done = []
            back = jnp.dot(unperm, wide, preferred_element_type=F32)
            for f in range(facets):
                for c in range(chans):
                    at = (f * chans + c) * comps
                    out_ref[f, c, :, (s - 1) * per_slot : (s + 1) * per_slot] = back[
                        at : at + comps, :
                    ].astype(BF16)

    sent = send.at[pl.ds(0, (n - 1) * slab), :]
    pltpu.make_async_copy(sent, sent, send_sem).wait()


def shards(gains, visibilities, first_station, second_station, filled_row_count, facet_dir):
    n = lax.axis_size(("bt", "pol"))
    pols = lax.axis_size("pol")
    facets, chans, comps, rows = visibilities.shape
    slots = GAIN_SLOT_COUNT
    tiles = (slots // 2) * chans + (chans + 1) // 2
    total = facets * chans * comps
    anywhere = pl.BlockSpec(memory_space=pltpu.HBM)
    return pl.pallas_call(
        functools.partial(kernel, n, pols),
        out_shape=pltpu.VMEM(visibilities.shape, BF16),
        in_specs=[anywhere] * 6,
        out_specs=pl.BlockSpec(memory_space=pltpu.VMEM),
        scratch_shapes=[
            pltpu.VMEM(gains.shape, F32),
            pltpu.VMEM(visibilities.shape, BF16),
            pltpu.VMEM((2, slots, rows // slots), jnp.int32),
            pltpu.SMEM(filled_row_count.shape, jnp.int32),
            pltpu.SMEM(facet_dir.shape, jnp.int32),
            pltpu.VMEM((n * tiles * COMPS, LANES), F32),
            pltpu.VMEM((n * tiles * COMPS, LANES), F32),
            pltpu.VMEM((slots, 2 * LANES, 2 * (rows // slots)), BF16),
            pltpu.VMEM((total, rows), F32),
            pltpu.SemaphoreType.DMA((5,)),
            pltpu.SemaphoreType.DMA,
            pltpu.SemaphoreType.DMA,
        ],
        compiler_params=pltpu.CompilerParams(collective_id=0, has_side_effects=True),
        name="jones",
    )(
        gains,
        visibilities,
        first_station.reshape(slots, rows // slots),
        second_station.reshape(slots, rows // slots),
        filled_row_count,
        facet_dir,
    )


def solution(mesh):
    return jax.shard_map(
        shards,
        mesh=mesh,
        in_specs=(
            P(("obs", "bt", "pol"), "freq", None, None),
            P("obs", "freq", None, ("bt", "pol")),
            P(("obs", "bt", "pol")),
            P(("obs", "bt", "pol")),
            P(("obs", "bt", "pol")),
            P("obs"),
        ),
        out_specs=P("obs", "freq", None, ("bt", "pol")),
        check_vma=False,
    )
```
